16 devices in a mesh: tp: 2 (over z), dp: 8 (over y, x, core).
Axes of the slice: x: 2, y: 2, z: 2, core: 2. Of those that a mesh axis runs over, the one named last changes fastest.
Arguments:
- h_main: bfloat16 [8, 512, 4096], P('dp')
- h_mtp: bfloat16 [8, 512, 4096], P('dp')
- labels_main: int32 [8, 512], P('dp')
- labels_mtp: int32 [8, 512], P('dp')
- weight_main: float32 [8, 512], P('dp')
- weight_mtp: float32 [8, 512], P('dp')
- gain_final: float32 [4096], replicated
- gain_mtp: float32 [4096], replicated
- w_out: bfloat16 [4096, 32256], P(None, 'tp')
Outputs:
- output 1: float32 [], replicated
- output 2: bfloat16 [8, 512, 4096], P('dp')
- output 3: bfloat16 [8, 512, 4096], P('dp')
- output 4: float32 [4096, 32256], P('dp', 'tp')
- output 5: float32 [4096], replicated
- output 6: float32 [4096], replicated
All inputs are finite; a program needn't handle non-finite values.
Results may differ from the reference program's by a relative error of at most 0.00844935.
Values sent between devices are 32-bit elements.
A program may use at most 1 GiB of HBM per device.

```python
import jax
import jax.numpy as jnp
from jax import lax

BATCH_ALL = 8
SEQ_LEN = 512
D_MODEL = 4096
VOCAB_SIZE = 32256
TP_SHARDS = 2
ROW_BLOCK = 256
SHARD_VOCAB = VOCAB_SIZE // TP_SHARDS
ROWS_ALL = BATCH_ALL * SEQ_LEN
NUM_BLOCKS = ROWS_ALL // ROW_BLOCK
NORM_EPS = 1e-6
MTP_LAMBDA = 0.3
LOGIT_SCALE = 3.0


def setup_inputs(seed: int = 0) -> dict:
    key_list = jax.random.split(jax.random.key(seed), 7)
    h_main = jax.random.normal(key_list[0], (BATCH_ALL, SEQ_LEN, D_MODEL), jnp.float32).astype(jnp.bfloat16)
    h_mtp = jax.random.normal(key_list[1], (BATCH_ALL, SEQ_LEN, D_MODEL), jnp.float32).astype(jnp.bfloat16)
    tokens = jax.random.randint(key_list[2], (BATCH_ALL, SEQ_LEN + 2), 0, VOCAB_SIZE, jnp.int32)
    tokens = tokens.at[0, 1].set(VOCAB_SIZE - 1).at[0, 2].set(0)
    lengths = jax.random.randint(key_list[3], (BATCH_ALL,), SEQ_LEN // 4, SEQ_LEN + 1, jnp.int32)
    lengths = lengths.at[0].set(SEQ_LEN).at[BATCH_ALL - 1].set(SEQ_LEN // 4)
    positions = jnp.arange(SEQ_LEN, dtype=jnp.int32)[None, :]
    weight_main = (positions < lengths[:, None]).astype(jnp.float32)
    weight_mtp = (positions < lengths[:, None] - 1).astype(jnp.float32)
    gain_final = 1.0 + 0.2 * jax.random.normal(key_list[4], (D_MODEL,), jnp.float32)
    gain_mtp = 1.0 + 0.2 * jax.random.normal(key_list[5], (D_MODEL,), jnp.float32)
    w_out = (jax.random.normal(key_list[6], (D_MODEL, VOCAB_SIZE), jnp.float32) * (LOGIT_SCALE * D_MODEL ** -0.5)).astype(jnp.bfloat16)
    return {"h_main": h_main, "h_mtp": h_mtp, "labels_main": tokens[:, 1:SEQ_LEN + 1], "labels_mtp": tokens[:, 2:], "weight_main": weight_main, "weight_mtp": weight_mtp, "gain_final": gain_final, "gain_mtp": gain_mtp, "w_out": w_out}


def norm_apply(x_rows, gain_vec):
    return x_rows * lax.rsqrt(jnp.mean(x_rows * x_rows, axis=-1, keepdims=True) + NORM_EPS) * gain_vec


def reference(h_main, h_mtp, labels_main, labels_mtp, weight_main, weight_mtp, gain_final, gain_mtp, w_out):
    coef_main = 1.0 / jnp.sum(weight_main)
    coef_mtp = MTP_LAMBDA / jnp.sum(weight_mtp)
    x_blocks = jnp.stack([h_main, h_mtp]).astype(jnp.float32).reshape(2 * NUM_BLOCKS, ROW_BLOCK, D_MODEL)
    label_blocks = jnp.stack([labels_main, labels_mtp]).reshape(2 * NUM_BLOCKS, ROW_BLOCK)
    weight_blocks = jnp.stack([weight_main * coef_main, weight_mtp * coef_mtp]).reshape(2 * NUM_BLOCKS, ROW_BLOCK)
    gain_blocks = jnp.repeat(jnp.stack([gain_final, gain_mtp]), NUM_BLOCKS, axis=0)
    w_shards = w_out.reshape(D_MODEL, TP_SHARDS, SHARD_VOCAB).transpose(1, 0, 2)

    def shard_product(operand_pair):
        grad_shard, w_shard = operand_pair
        return jnp.dot(grad_shard, w_shard.T, preferred_element_type=jnp.float32).astype(jnp.bfloat16)

    def block_step(grad_w, block_data):
        x_rows, labels, row_w, gain_vec = block_data
        u_rows = norm_apply(x_rows, gain_vec).astype(jnp.bfloat16)
        logits = jnp.dot(u_rows, w_out, preferred_element_type=jnp.float32)
        row_max = jnp.max(logits, axis=-1, keepdims=True)
        log_norm = row_max + jnp.log(jnp.sum(jnp.exp(logits - row_max), axis=-1, keepdims=True))
        onehot = jax.nn.one_hot(labels, VOCAB_SIZE, dtype=jnp.float32)
        target = jnp.sum(logits * onehot, axis=-1)
        loss_part = jnp.sum(row_w * (log_norm[:, 0] - target))
        grad_z = (row_w[:, None] * (jnp.exp(logits - log_norm) - onehot)).astype(jnp.bfloat16)
        grad_w = grad_w + lax.dot_general(u_rows, grad_z, (((0,), (0,)), ((), ())), preferred_element_type=jnp.float32)
        grad_split = grad_z.reshape(ROW_BLOCK, TP_SHARDS, SHARD_VOCAB).transpose(1, 0, 2)
        partials = lax.map(shard_product, (grad_split, w_shards))
        grad_u = jnp.sum(partials.astype(jnp.float32), axis=0)
        _, norm_vjp = jax.vjp(norm_apply, x_rows, gain_vec)
        grad_x, grad_gain = norm_vjp(grad_u)
        return grad_w, (loss_part, grad_x.astype(jnp.bfloat16), grad_gain)

    grad_w, outputs = lax.scan(block_step, jnp.zeros((D_MODEL, VOCAB_SIZE), jnp.float32), (x_blocks, label_blocks, weight_blocks, gain_blocks))
    loss_parts, grad_x, grad_gain = outputs
    grad_h = grad_x.reshape(2, BATCH_ALL, SEQ_LEN, D_MODEL)
    gain_grads = grad_gain.reshape(2, NUM_BLOCKS, D_MODEL).sum(axis=1)
    return (jnp.sum(loss_parts), grad_h[0], grad_h[1], grad_w, gain_grads[0], gain_grads[1])
```

```python
import jax
import jax.numpy as jnp
from jax import lax
from jax.sharding import PartitionSpec as P


NORM_EPS = 1e-6
MTP_LAMBDA = 0.3
CHUNKS = 4


def solution(mesh):
    n_dp = mesh.shape['dp']
    n_tp = mesh.shape['tp']

    def layer_step(h_main, h_mtp, labels_main, labels_mtp, weight_main, weight_mtp, gain_final, gain_mtp, w_out):
        batch_loc, seq_len, d_model = h_main.shape
        shard_vocab = w_out.shape[1]
        rows = batch_loc * seq_len
        half = rows // n_tp
        dp_rank = lax.axis_index('dp')
        tp_rank = lax.axis_index('tp')
        gains = (gain_final[None, :], gain_mtp[None, :])

        normed, gathered = [], []
        for h in (h_main, h_mtp):
            x = h.reshape(rows, d_model).astype(jnp.float32)
            inv = lax.rsqrt(jnp.mean(x * x, axis=-1, keepdims=True) + NORM_EPS)
            n = x * inv
            normed.append(n)
            gathered.append(lax.all_gather(lax.dynamic_slice_in_dim(n, tp_rank * half, half, 0), ('tp', 'dp'), axis=0, tiled=True))

        vocab_start = tp_rank * shard_vocab
        column = jnp.arange(shard_vocab, dtype=jnp.int32)[None, :]
        u_own = [(n * g).astype(jnp.bfloat16) for n, g in zip(normed, gains)]
        labels_own = [l.reshape(rows) for l in (labels_main, labels_mtp)]
        weights_own = [w.reshape(rows) for w in (weight_main, weight_mtp)]
        u_rows = jnp.concatenate(u_own, axis=0)
        local_labels = jnp.concatenate(labels_own) - vocab_start
        logits = jnp.dot(u_rows, w_out, preferred_element_type=jnp.float32)
        row_max = jnp.max(logits, axis=-1)
        is_target = column == local_labels[:, None]
        row_sum = jnp.sum(jnp.exp(logits - row_max[:, None]), axis=-1)
        row_target = jnp.sum(jnp.where(is_target, logits, 0.0), axis=-1)

        stats = jnp.stack([row_max, row_sum, row_target, jnp.concatenate(labels_own).astype(jnp.float32), jnp.concatenate(weights_own)])
        stats = lax.all_gather(stats, ('tp', 'dp'), axis=0, tiled=False).reshape(n_tp, n_dp, 5, 2, rows)
        all_max = jnp.max(stats[:, :, 0], axis=0)
        all_sum = jnp.sum(stats[:, :, 1] * jnp.exp(stats[:, :, 0] - all_max[None]), axis=0)
        all_lse = all_max + jnp.log(all_sum)
        all_target = jnp.sum(stats[:, :, 2], axis=0)
        all_labels = stats[0, :, 3].astype(jnp.int32)
        all_weights = stats[0, :, 4]
        coefs = jnp.array([1.0, MTP_LAMBDA], jnp.float32) / jnp.sum(all_weights, axis=(0, 2))
        all_row_w = all_weights * coefs[None, :, None]
        loss_total = jnp.sum(all_row_w * (all_lse - all_target))

        own_lse = lax.dynamic_index_in_dim(all_lse, dp_rank, 0, keepdims=False).reshape(2 * rows)
        own_row_w = lax.dynamic_index_in_dim(all_row_w, dp_rank, 0, keepdims=False).reshape(2 * rows)
        probs = jnp.exp(logits - own_lse[:, None])
        grad_z = (own_row_w[:, None] * jnp.where(is_target, probs - 1.0, probs)).astype(jnp.bfloat16)
        grad_u = []
        for which in range(2):
            part = lax.dot_general(grad_z[which * rows:(which + 1) * rows], w_out, (((1,), (1,)), ((), ())), preferred_element_type=jnp.float32).astype(jnp.bfloat16).astype(jnp.float32)
            grad_u.append((part, lax.ppermute(part, 'tp', [(i, n_tp - 1 - i) for i in range(n_tp)])))

        width = -(-shard_vocab // (n_dp * 256)) * 256
        col_unit = jnp.minimum(dp_rank * (width // 256), (shard_vocab - width) // 256)
        w_slice = lax.dynamic_slice_in_dim(w_out, col_unit * 256, width, 1)
        slice_start = vocab_start + col_unit * 256

        def token_order(a):
            return a.reshape(n_dp, n_tp, half).transpose(1, 0, 2).reshape(n_dp * rows)

        def slice_grad(which, u_all, cols, start):
            z = jnp.dot(u_all, cols, preferred_element_type=jnp.float32)
            hit = (jnp.arange(cols.shape[1], dtype=jnp.int32)[None, :] + start) == token_order(all_labels[:, which])[:, None]
            p = jnp.exp(z - token_order(all_lse[:, which])[:, None])
            e = (token_order(all_row_w[:, which])[:, None] * jnp.where(hit, p - 1.0, p)).astype(jnp.bfloat16)
            return lax.dot_general(u_all, e, (((0,), (0,)), ((), ())), preferred_element_type=jnp.float32)

        u_all = [(n * g).astype(jnp.bfloat16) for n, g in zip(gathered, gains)]
        grad_main = slice_grad(0, u_all[0], w_slice, slice_start)
        d_loc = d_model // n_dp
        grad_w = jnp.zeros((d_loc, shard_vocab), jnp.float32)
        cw = width // CHUNKS
        for q in range(CHUNKS):
            cols = w_slice[:, q * cw:(q + 1) * cw]
            part = grad_main[:, q * cw:(q + 1) * cw] + slice_grad(1, u_all[1], cols, slice_start + q * cw)
            sends = lax.optimization_barrier([lax.dynamic_slice(part, ((dp_rank ^ k) * d_loc, 0), (d_loc, cw)) for k in range(n_dp)])
            for k, block in enumerate(sends):
                if k:
                    block = lax.ppermute(block, 'dp', [(i, i ^ k) for i in range(n_dp)])
                peer_unit = jnp.minimum((dp_rank ^ k) * (width // 256), (shard_vocab - width) // 256)
                grad_w = lax.dynamic_update_slice(grad_w, block, (0, (peer_unit + q * cw // 256) * 256))

        grads_h, gain_parts = [], []
        for which, h in enumerate((h_main, h_mtp)):
            h, part, other = lax.optimization_barrier((h, *grad_u[which]))
            x = h.reshape(rows, d_model).astype(jnp.float32)
            inv = lax.rsqrt(jnp.mean(x * x, axis=-1, keepdims=True) + NORM_EPS)
            n = x * inv
            du = part + other
            grad_normed = du * gains[which]
            gain_parts.append(jnp.sum(du * n, axis=0))
            grad_x = inv * (grad_normed - n * jnp.mean(grad_normed * n, axis=-1, keepdims=True))
            grads_h.append(grad_x.astype(jnp.bfloat16).reshape(batch_loc, seq_len, d_model))
        grad_gain = lax.psum(jnp.stack(gain_parts), 'dp')
        return loss_total, grads_h[0], grads_h[1], grad_w, grad_gain[0], grad_gain[1]


    row_spec = P('dp', None)
    return jax.shard_map(layer_step, mesh=mesh, in_specs=(P('dp', None, None), P('dp', None, None), row_spec, row_spec, row_spec, row_spec, P(None), P(None), P(None, 'tp')), out_specs=(P(), P('dp', None, None), P('dp', None, None), P('dp', 'tp'), P(None), P(None)), check_vma=False)
```

```python
import jax
import jax.numpy as jnp
from jax import lax
from jax.sharding import PartitionSpec as P


NORM_EPS = 1e-6
MTP_LAMBDA = 0.3
CHUNKS = 4


def solution(mesh):
    n_dp = mesh.shape['dp']
    n_tp = mesh.shape['tp']

    def layer_step(h_main, h_mtp, labels_main, labels_mtp, weight_main, weight_mtp, gain_final, gain_mtp, w_out):
        batch_loc, seq_len, d_model = h_main.shape
        shard_vocab = w_out.shape[1]
        rows = batch_loc * seq_len
        half = rows // n_tp
        dp_rank = lax.axis_index('dp')
        tp_rank = lax.axis_index('tp')
        gains = (gain_final[None, :], gain_mtp[None, :])

        normed, gathered = [], []
        for h in (h_main, h_mtp):
            x = h.reshape(rows, d_model).astype(jnp.float32)
            inv = lax.rsqrt(jnp.mean(x * x, axis=-1, keepdims=True) + NORM_EPS)
            n = x * inv
            normed.append(n)
            gathered.append(lax.all_gather(lax.dynamic_slice_in_dim(n, tp_rank * half, half, 0), ('tp', 'dp'), axis=0, tiled=True))

        vocab_start = tp_rank * shard_vocab
        column = jnp.arange(shard_vocab, dtype=jnp.int32)[None, :]
        u_own = [(n * g).astype(jnp.bfloat16) for n, g in zip(normed, gains)]
        labels_own = [l.reshape(rows) for l in (labels_main, labels_mtp)]
        weights_own = [w.reshape(rows) for w in (weight_main, weight_mtp)]
        u_rows = jnp.concatenate(u_own, axis=0)
        local_labels = jnp.concatenate(labels_own) - vocab_start
        logits = jnp.dot(u_rows, w_out, preferred_element_type=jnp.float32)
        row_max = jnp.max(logits, axis=-1)
        is_target = column == local_labels[:, None]
        row_sum = jnp.sum(jnp.exp(logits - row_max[:, None]), axis=-1)
        row_target = jnp.sum(jnp.where(is_target, logits, 0.0), axis=-1)

        stats = jnp.stack([row_max, row_sum, row_target, jnp.concatenate(labels_own).astype(jnp.float32), jnp.concatenate(weights_own)])
        stats = lax.all_gather(stats, ('tp', 'dp'), axis=0, tiled=False).reshape(n_tp, n_dp, 5, 2, rows)
        all_max = jnp.max(stats[:, :, 0], axis=0)
        all_sum = jnp.sum(stats[:, :, 1] * jnp.exp(stats[:, :, 0] - all_max[None]), axis=0)
        all_lse = all_max + jnp.log(all_sum)
        all_target = jnp.sum(stats[:, :, 2], axis=0)
        all_labels = stats[0, :, 3].astype(jnp.int32)
        all_weights = stats[0, :, 4]
        coefs = jnp.array([1.0, MTP_LAMBDA], jnp.float32) / jnp.sum(all_weights, axis=(0, 2))
        all_row_w = all_weights * coefs[None, :, None]
        loss_total = jnp.sum(all_row_w * (all_lse - all_target))

        own_lse = lax.dynamic_index_in_dim(all_lse, dp_rank, 0, keepdims=False).reshape(2 * rows)
        own_row_w = lax.dynamic_index_in_dim(all_row_w, dp_rank, 0, keepdims=False).reshape(2 * rows)
        probs = jnp.exp(logits - own_lse[:, None])
        grad_z = (own_row_w[:, None] * jnp.where(is_target, probs - 1.0, probs)).astype(jnp.bfloat16)
        grad_u, gain_parts = [], []
        for which in range(2):
            part = lax.dot_general(grad_z[which * rows:(which + 1) * rows], w_out, (((1,), (1,)), ((), ())), preferred_element_type=jnp.float32).astype(jnp.bfloat16).astype(jnp.float32)
            h, part = lax.optimization_barrier(((h_main, h_mtp)[which], part))
            x = h.reshape(rows, d_model).astype(jnp.float32)
            gain_parts.append(jnp.sum(part * (x * lax.rsqrt(jnp.mean(x * x, axis=-1, keepdims=True) + NORM_EPS)), axis=0))
            grad_u.append((part, lax.ppermute(part, 'tp', [(i, n_tp - 1 - i) for i in range(n_tp)])))
        grad_gain = jnp.stack(gain_parts)
        for axis, size in (('dp', n_dp), ('tp', n_tp)):
            bit = 1
            while bit < size:
                grad_gain = grad_gain + lax.ppermute(grad_gain, axis, [(i, i ^ bit) for i in range(size)])
                bit *= 2

        width = -(-shard_vocab // (n_dp * 256)) * 256
        col_unit = jnp.minimum(dp_rank * (width // 256), (shard_vocab - width) // 256)
        w_slice = lax.dynamic_slice_in_dim(w_out, col_unit * 256, width, 1)
        slice_start = vocab_start + col_unit * 256

        def token_order(a):
            return a.reshape(n_dp, n_tp, half).transpose(1, 0, 2).reshape(n_dp * rows)

        def slice_grad(which, u_all, cols, start):
            z = jnp.dot(u_all, cols, preferred_element_type=jnp.float32)
            hit = (jnp.arange(cols.shape[1], dtype=jnp.int32)[None, :] + start) == token_order(all_labels[:, which])[:, None]
            p = jnp.exp(z - token_order(all_lse[:, which])[:, None])
            e = (token_order(all_row_w[:, which])[:, None] * jnp.where(hit, p - 1.0, p)).astype(jnp.bfloat16)
            return lax.dot_general(u_all, e, (((0,), (0,)), ((), ())), preferred_element_type=jnp.float32)

        u_all = [(n * g).astype(jnp.bfloat16) for n, g in zip(gathered, gains)]
        d_loc = d_model // n_dp
        grad_w = jnp.zeros((d_loc, shard_vocab), jnp.float32)
        cw = width // CHUNKS
        for q in range(CHUNKS):
            cols = w_slice[:, q * cw:(q + 1) * cw]
            part = slice_grad(0, u_all[0], cols, slice_start + q * cw)
            part = part + slice_grad(1, u_all[1], cols, slice_start + q * cw)
            sends = lax.optimization_barrier([lax.dynamic_slice(part, ((dp_rank ^ k) * d_loc, 0), (d_loc, cw)) for k in range(n_dp)])
            for k, block in enumerate(sends):
                if k:
                    block = lax.ppermute(block, 'dp', [(i, i ^ k) for i in range(n_dp)])
                peer_unit = jnp.minimum((dp_rank ^ k) * (width // 256), (shard_vocab - width) // 256)
                grad_w = lax.dynamic_update_slice(grad_w, block, (0, (peer_unit + q * cw // 256) * 256))

        grads_h = []
        for which, h in enumerate((h_main, h_mtp)):
            h, part, other = lax.optimization_barrier((h, *grad_u[which]))
            x = h.reshape(rows, d_model).astype(jnp.float32)
            inv = lax.rsqrt(jnp.mean(x * x, axis=-1, keepdims=True) + NORM_EPS)
            n = x * inv
            du = part + other
            grad_normed = du * gains[which]
            grad_x = inv * (grad_normed - n * jnp.mean(grad_normed * n, axis=-1, keepdims=True))
            grads_h.append(grad_x.astype(jnp.bfloat16).reshape(batch_loc, seq_len, d_model))
        return loss_total, grads_h[0], grads_h[1], grad_w, grad_gain[0], grad_gain[1]

    row_spec = P('dp', None)
    return jax.shard_map(layer_step, mesh=mesh, in_specs=(P('dp', None, None), P('dp', None, None), row_spec, row_spec, row_spec, row_spec, P(None), P(None), P(None, 'tp')), out_specs=(P(), P('dp', None, None), P('dp', None, None), P('dp', 'tp'), P(None), P(None)), check_vma=False)
```

```python
import jax
import jax.numpy as jnp
from jax import lax
from jax.sharding import PartitionSpec as P


NORM_EPS = 1e-6
MTP_LAMBDA = 0.3
UNIT = 256
CHUNKS = (2, 2, 2, 2)


def solution(mesh):
    n_dp = mesh.shape['dp']
    n_tp = mesh.shape['tp']

    def layer_step(h_main, h_mtp, labels_main, labels_mtp, weight_main, weight_mtp, gain_final, gain_mtp, w_out):
        batch_loc, seq_len, d_model = h_main.shape
        shard_vocab = w_out.shape[1]
        rows = batch_loc * seq_len
        half = rows // n_tp
        dp_rank = lax.axis_index('dp')
        tp_rank = lax.axis_index('tp')
        gains = (gain_final[None, :], gain_mtp[None, :])

        def normalise(h):
            x = h.reshape(-1, d_model).astype(jnp.float32)
            inv = lax.rsqrt(jnp.mean(x * x, axis=-1, keepdims=True) + NORM_EPS)
            return x * inv, inv

        gathered = []
        for h in (h_main, h_mtp):
            h_half = lax.optimization_barrier(lax.dynamic_slice_in_dim(h.reshape(rows, d_model), tp_rank * half, half, 0))
            gathered.append(lax.all_gather(normalise(h_half)[0], ('tp', 'dp'), axis=0, tiled=True))
        normed = [normalise(h)[0] for h in (h_main, h_mtp)]

        vocab_start = tp_rank * shard_vocab
        column = jnp.arange(shard_vocab, dtype=jnp.int32)[None, :]
        u_own = [(n * g).astype(jnp.bfloat16) for n, g in zip(normed, gains)]
        labels_own = [l.reshape(rows) for l in (labels_main, labels_mtp)]
        weights_own = [w.reshape(rows) for w in (weight_main, weight_mtp)]
        u_rows = jnp.concatenate(u_own, axis=0)
        local_labels = jnp.concatenate(labels_own) - vocab_start
        logits = jnp.dot(u_rows, w_out, preferred_element_type=jnp.float32)
        row_max = jnp.max(logits, axis=-1)
        is_target = column == local_labels[:, None]
        row_sum = jnp.sum(jnp.exp(logits - row_max[:, None]), axis=-1)
        row_target = jnp.sum(jnp.where(is_target, logits, 0.0), axis=-1)

        stats = jnp.stack([row_max, row_sum, row_target, jnp.concatenate(labels_own).astype(jnp.float32), jnp.concatenate(weights_own)])
        stats = lax.all_gather(stats, ('tp', 'dp'), axis=0, tiled=False).reshape(n_tp, n_dp, 5, 2, rows)
        all_max = jnp.max(stats[:, :, 0], axis=0)
        all_sum = jnp.sum(stats[:, :, 1] * jnp.exp(stats[:, :, 0] - all_max[None]), axis=0)
        all_lse = all_max + jnp.log(all_sum)
        all_target = jnp.sum(stats[:, :, 2], axis=0)
        all_labels = stats[0, :, 3].astype(jnp.int32)
        all_weights = stats[0, :, 4]
        coefs = jnp.array([1.0, MTP_LAMBDA], jnp.float32) / jnp.sum(all_weights, axis=(0, 2))
        all_row_w = all_weights * coefs[None, :, None]
        loss_total = jnp.sum(all_row_w * (all_lse - all_target))

        own_lse = lax.dynamic_index_in_dim(all_lse, dp_rank, 0, keepdims=False).reshape(2 * rows)
        own_row_w = lax.dynamic_index_in_dim(all_row_w, dp_rank, 0, keepdims=False).reshape(2 * rows)
        probs = jnp.exp(logits - own_lse[:, None])
        grad_z = (own_row_w[:, None] * jnp.where(is_target, probs - 1.0, probs)).astype(jnp.bfloat16)
        grad_u, gain_parts = [], []
        for which in range(2):
            part = lax.dot_general(grad_z[which * rows:(which + 1) * rows], w_out, (((1,), (1,)), ((), ())), preferred_element_type=jnp.float32).astype(jnp.bfloat16).astype(jnp.float32)
            h, part = lax.optimization_barrier(((h_main, h_mtp)[which], part))
            gain_parts.append(jnp.sum(part * normalise(h)[0], axis=0))
            grad_u.append((part, lax.ppermute(part, 'tp', [(i, n_tp - 1 - i) for i in range(n_tp)])))
        grad_gain = jnp.stack(gain_parts)
        for axis, size in (('dp', n_dp), ('tp', n_tp)):
            bit = 1
            while bit < size:
                grad_gain = grad_gain + lax.ppermute(grad_gain, axis, [(i, i ^ bit) for i in range(size)])
                bit *= 2

        units = sum(CHUNKS)
        width = units * UNIT
        assert n_dp * width >= shard_vocab and shard_vocab % UNIT == 0

        def first_unit(rank):
            return jnp.minimum(rank * units, shard_vocab // UNIT - units)

        w_slice = lax.dynamic_slice_in_dim(w_out, first_unit(dp_rank) * UNIT, width, 1)
        slice_start = vocab_start + first_unit(dp_rank) * UNIT

        def token_order(a):
            return a.reshape(n_dp, n_tp, half).transpose(1, 0, 2).reshape(n_dp * rows)

        def slice_grad(which, u_all, cols, start):
            z = jnp.dot(u_all, cols, preferred_element_type=jnp.float32)
            hit = (jnp.arange(cols.shape[1], dtype=jnp.int32)[None, :] + start) == token_order(all_labels[:, which])[:, None]
            p = jnp.exp(z - token_order(all_lse[:, which])[:, None])
            e = (token_order(all_row_w[:, which])[:, None] * jnp.where(hit, p - 1.0, p)).astype(jnp.bfloat16)
            return lax.dot_general(u_all, e, (((0,), (0,)), ((), ())), preferred_element_type=jnp.float32)

        u_all = [(n * g).astype(jnp.bfloat16) for n, g in zip(gathered, gains)]
        d_loc = d_model // n_dp
        grad_w = jnp.zeros((d_loc, shard_vocab), jnp.float32)
        grad_main = slice_grad(0, u_all[0], w_slice, slice_start)
        for q, chunk in enumerate(CHUNKS):
            done = sum(CHUNKS[:q])
            lo, cw = done * UNIT, chunk * UNIT
            cols = w_slice[:, lo:lo + cw]
            part = grad_main[:, lo:lo + cw] + slice_grad(1, u_all[1], cols, slice_start + lo)
            sends = lax.optimization_barrier([lax.dynamic_slice(part, ((dp_rank ^ k) * d_loc, 0), (d_loc, cw)) for k in range(n_dp)])
            for k, block in enumerate(sends):
                if k:
                    block = lax.ppermute(block, 'dp', [(i, i ^ k) for i in range(n_dp)])
                grad_w = lax.dynamic_update_slice(grad_w, block, (0, (first_unit(dp_rank ^ k) + done) * UNIT))

        grads_h = []
        for which, h in enumerate((h_main, h_mtp)):
            h, part, other = lax.optimization_barrier((h, *grad_u[which]))
            n, inv = normalise(h)
            du = part + other
            grad_normed = du * gains[which]
            grad_x = inv * (grad_normed - n * jnp.mean(grad_normed * n, axis=-1, keepdims=True))
            grads_h.append(grad_x.astype(jnp.bfloat16).reshape(batch_loc, seq_len, d_model))
        return loss_total, grads_h[0], grads_h[1], grad_w, grad_gain[0], grad_gain[1]


    row_spec = P('dp', None)
    return jax.shard_map(layer_step, mesh=mesh, in_specs=(P('dp', None, None), P('dp', None, None), row_spec, row_spec, row_spec, row_spec, P(None), P(None), P(None, 'tp')), out_specs=(P(), P('dp', None, None), P('dp', None, None), P('dp', 'tp'), P(None), P(None)), check_vma=False)
```

```python
import jax
import jax.numpy as jnp
from jax import lax
from jax.sharding import PartitionSpec as P


NORM_EPS = 1e-6
MTP_LAMBDA = 0.3
UNIT = 256
CHUNKS = (2, 3, 2, 1)


def solution(mesh):
    n_dp = mesh.shape['dp']
    n_tp = mesh.shape['tp']

    def layer_step(h_main, h_mtp, labels_main, labels_mtp, weight_main, weight_mtp, gain_final, gain_mtp, w_out):
        batch_loc, seq_len, d_model = h_main.shape
        shard_vocab = w_out.shape[1]
        rows = batch_loc * seq_len
        half = rows // n_tp
        dp_rank = lax.axis_index('dp')
        tp_rank = lax.axis_index('tp')
        gains = (gain_final[None, :], gain_mtp[None, :])

        def normalise(h):
            x = h.reshape(-1, d_model).astype(jnp.float32)
            inv = lax.rsqrt(jnp.mean(x * x, axis=-1, keepdims=True) + NORM_EPS)
            return x * inv, inv

        gathered = []
        for h in (h_main, h_mtp):
            h_half = lax.optimization_barrier(lax.dynamic_slice_in_dim(h.reshape(rows, d_model), tp_rank * half, half, 0))
            gathered.append(lax.all_gather(normalise(h_half)[0], ('tp', 'dp'), axis=0, tiled=True))
        normed = [normalise(h)[0] for h in (h_main, h_mtp)]

        vocab_start = tp_rank * shard_vocab
        column = jnp.arange(shard_vocab, dtype=jnp.int32)[None, :]
        u_own = [(n * g).astype(jnp.bfloat16) for n, g in zip(normed, gains)]
        labels_own = [l.reshape(rows) for l in (labels_main, labels_mtp)]
        weights_own = [w.reshape(rows) for w in (weight_main, weight_mtp)]
        u_rows = jnp.concatenate(u_own, axis=0)
        local_labels = jnp.concatenate(labels_own) - vocab_start
        logits = jnp.dot(u_rows, w_out, preferred_element_type=jnp.float32)
        row_max = jnp.max(logits, axis=-1)
        is_target = column == local_labels[:, None]
        row_sum = jnp.sum(jnp.exp(logits - row_max[:, None]), axis=-1)
        row_target = jnp.sum(jnp.where(is_target, logits, 0.0), axis=-1)

        stats = jnp.stack([row_max, row_sum, row_target, jnp.concatenate(labels_own).astype(jnp.float32), jnp.concatenate(weights_own)])
        stats = lax.all_gather(stats, ('tp', 'dp'), axis=0, tiled=False).reshape(n_tp, n_dp, 5, 2, rows)
        all_max = jnp.max(stats[:, :, 0], axis=0)
        all_sum = jnp.sum(stats[:, :, 1] * jnp.exp(stats[:, :, 0] - all_max[None]), axis=0)
        all_lse = all_max + jnp.log(all_sum)
        all_target = jnp.sum(stats[:, :, 2], axis=0)
        all_labels = stats[0, :, 3].astype(jnp.int32)
        all_weights = stats[0, :, 4]
        coefs = jnp.array([1.0, MTP_LAMBDA], jnp.float32) / jnp.sum(all_weights, axis=(0, 2))
        all_row_w = all_weights * coefs[None, :, None]
        loss_total = jnp.sum(all_row_w * (all_lse - all_target))

        own_lse = lax.dynamic_index_in_dim(all_lse, dp_rank, 0, keepdims=False).reshape(2 * rows)
        own_row_w = lax.dynamic_index_in_dim(all_row_w, dp_rank, 0, keepdims=False).reshape(2 * rows)
        probs = jnp.exp(logits - own_lse[:, None])
        grad_z = (own_row_w[:, None] * jnp.where(is_target, probs - 1.0, probs)).astype(jnp.bfloat16)
        pieces = ((0, 0, rows), (1, 0, rows))
        grad_u, gain_parts = [], [0.0, 0.0]
        for which, row, count in pieces:
            part = lax.dot_general(grad_z[which * rows + row:which * rows + row + count], w_out, (((1,), (1,)), ((), ())), preferred_element_type=jnp.float32).astype(jnp.bfloat16).astype(jnp.float32)
            h, part = lax.optimization_barrier(((h_main, h_mtp)[which].reshape(rows, d_model)[row:row + count], part))
            gain_parts[which] += jnp.sum(part * normalise(h)[0], axis=0)
            grad_u.append((part, lax.ppermute(part, 'tp', [(j, n_tp - 1 - j) for j in range(n_tp)])))
        grad_gain = jnp.stack(gain_parts)
        for axis, size in (('dp', n_dp), ('tp', n_tp)):
            bit = 1
            while bit < size:
                grad_gain = grad_gain + lax.ppermute(grad_gain, axis, [(i, i ^ bit) for i in range(size)])
                bit *= 2

        units = sum(CHUNKS)
        width = units * UNIT
        assert n_dp * width >= shard_vocab and shard_vocab % UNIT == 0

        def first_unit(rank):
            return jnp.minimum(rank * units, shard_vocab // UNIT - units)

        w_slice = lax.dynamic_slice_in_dim(w_out, first_unit(dp_rank) * UNIT, width, 1)
        slice_start = vocab_start + first_unit(dp_rank) * UNIT

        def token_order(a):
            return a.reshape(n_dp, n_tp, half).transpose(1, 0, 2).reshape(n_dp * rows)

        def rows_of(which, other):
            n, other = lax.optimization_barrier((gathered[which], other))
            return (n * gains[which]).astype(jnp.bfloat16), other

        def slice_dz(which, cols, start):
            z = jnp.dot(*rows_of(which, cols), preferred_element_type=jnp.float32)
            hit = (jnp.arange(cols.shape[1], dtype=jnp.int32)[None, :] + start) == token_order(all_labels[:, which])[:, None]
            p = jnp.exp(z - token_order(all_lse[:, which])[:, None])
            return (token_order(all_row_w[:, which])[:, None] * jnp.where(hit, p - 1.0, p)).astype(jnp.bfloat16)

        def slice_grad(which, e):
            return lax.dot_general(*rows_of(which, e), (((0,), (0,)), ((), ())), preferred_element_type=jnp.float32)

        d_loc = d_model // n_dp
        grad_w = jnp.zeros((d_loc, shard_vocab), jnp.float32)
        grad_main = slice_grad(0, slice_dz(0, w_slice, slice_start))
        dz_mtp, split = [], sum(CHUNKS[:2]) * UNIT
        for lo, hi in ((0, split), (split, width)):
            dz_mtp.append(slice_dz(1, w_slice[:, lo:hi], slice_start + lo))
        for q, chunk in enumerate(CHUNKS):
            done = sum(CHUNKS[:q])
            lo, cw = done * UNIT, chunk * UNIT
            dz = (dz_mtp[0][:, lo:] if lo < split else dz_mtp[1][:, lo - split:])[:, :cw]
            part = grad_main[:, lo:lo + cw] + slice_grad(1, dz)
            sends = lax.optimization_barrier([lax.dynamic_slice(part, ((dp_rank ^ k) * d_loc, 0), (d_loc, cw)) for k in range(n_dp)])
            for k, block in enumerate(sends):
                if k:
                    block = lax.ppermute(block, 'dp', [(i, i ^ k) for i in range(n_dp)])
                grad_w = lax.dynamic_update_slice(grad_w, block, (0, (first_unit(dp_rank ^ k) + done) * UNIT))

        grads_h = [[], []]
        for (which, row, count), (part, other) in zip(pieces, grad_u):
            h, part, other = lax.optimization_barrier(((h_main, h_mtp)[which].reshape(rows, d_model)[row:row + count], part, other))
            n, inv = normalise(h)
            grad_normed = (part + other) * gains[which]
            grad_x = inv * (grad_normed - n * jnp.mean(grad_normed * n, axis=-1, keepdims=True))
            grads_h[which].append(grad_x.astype(jnp.bfloat16))
        grads_h = [jnp.concatenate(g).reshape(batch_loc, seq_len, d_model) for g in grads_h]
        return loss_total, grads_h[0], grads_h[1], grad_w, grad_gain[0], grad_gain[1]


    row_spec = P('dp', None)
    return jax.shard_map(layer_step, mesh=mesh, in_specs=(P('dp', None, None), P('dp', None, None), row_spec, row_spec, row_spec, row_spec, P(None), P(None), P(None, 'tp')), out_specs=(P(), P('dp', None, None), P('dp', None, None), P('dp', 'tp'), P(None), P(None)), check_vma=False)
```
